32 devices in a mesh: gx: 4 (over y, x), gy: 4 (over z), gz: 2 (over core).
Axes of the slice: x: 2, y: 2, z: 4, core: 2. Of those that a mesh axis runs over, the one named last changes fastest.
Arguments:
- rhs: bfloat16 [2, 4096, 4096], P('gz', 'gx', 'gy'), may hold values from -40 to 40
- basis_x: bfloat16 [4096, 4096], P('gx', ('gy', 'gz')), may hold values from -0.125 to 0.125
- basis_y: bfloat16 [4096, 4096], P('gy', ('gx', 'gz')), may hold values from -0.125 to 0.125
- eig_x: float32 [4096], P('gx'), may hold values from 0.1 to 4
- eig_y: float32 [4096], P('gy'), may hold values from 0.1 to 4
- eig_z: float32 [2], P('gz'), may hold values from 0.1 to 4
Outputs:
- solution: bfloat16 [2, 4096, 4096], P('gz', 'gx', 'gy')
- energy: float32 [], replicated
The draws below stay inside these ranges and needn't reach their ends.
All inputs are finite; a program needn't handle non-finite values.
Results may differ from the reference program's by a relative error of at most 0.01.
Values may be sent and summed in bfloat16 or wider, within the bound.
No kernel may reach another device: no remote copies, remote signals or barrier semaphores. Data moves between devices by JAX's collectives and lax.ppermute only.
A program may use at most 128 MiB of HBM per device.

```python
import math
import jax
import jax.numpy as jnp

NX = 4096
NY = 4096
KZ = 2


def draw_rhs(key, part):
    first_key, second_key = jax.random.split(jax.random.fold_in(key, 17))
    position = jnp.arange(NX, dtype=jnp.float32) / NX
    rough = jnp.exp(jax.random.uniform(second_key, (NX,), jnp.float32, -0.7, 0.7))
    values = jnp.clip(jax.random.normal(first_key, (KZ, NX, NY), jnp.float32), -6.0, 6.0)
    trend = jnp.exp(jnp.log(3.0) * position)
    return (values * (trend * rough)[None, :, None]).astype(jnp.bfloat16)


def with_spikes(drawn, key, source, target, shards_of, factor):
    owner, partner = [(jnp.arange(drawn.shape[dim]) // (drawn.shape[dim] // shards_of)).reshape([-1 if axis == dim else 1 for axis in range(drawn.ndim)]) for dim in (source, target)]
    chosen = jax.random.permutation(key, shards_of)[partner]
    strong = (owner == chosen) | (owner == (partner + shards_of // 2) % shards_of)
    return jnp.where(strong, factor * drawn, drawn)


def levels(own_key, extent, shards, smallest, largest):
    gain = 1.0
    for dim, shards_of in shards:
        heights = jax.random.uniform(jax.random.fold_in(jax.random.fold_in(own_key, 6), dim), (shards_of,), jnp.float32, smallest / len(shards), largest / len(shards))
        gain = gain * jnp.repeat(jnp.exp(heights), extent[dim] // shards_of).reshape((-1,) + (1,) * (len(extent) - 1 - dim))
    return gain


def gaussian_with(key, extent, spread, bound, cuts, heavy, held_as=jnp.bfloat16):
    array = spread * jax.random.normal(key, extent, jnp.float32)
    if cuts:
        array = array * levels(key, extent, cuts, -0.22, 0.18)
    return jnp.clip(with_spikes(array, jax.random.fold_in(key, 3), *heavy), -bound, bound).astype(held_as)


def setup_inputs(seed: int = 0) -> dict:
    arg_keys = jax.random.split(jax.random.key(seed), 7)
    return {
        "rhs": draw_rhs(jax.random.fold_in(arg_keys[6], 71), 0),
        "basis_x": gaussian_with(arg_keys[1], (NX, NX), NX ** -0.5, 0.125, ((0, 4), (1, 8)), (0, 1, 8, 2.0)),
        "basis_y": gaussian_with(arg_keys[2], (NY, NY), NY ** -0.5, 0.125, ((0, 4), (1, 8)), (0, 1, 8, 2.0)),
        "eig_x": jnp.clip(jnp.exp(math.log(4.0) - 3.6888794 * jax.random.uniform(arg_keys[3], (NX,), jnp.float32) ** levels(arg_keys[3], (NX,), ((0, 4),), -0.2, 0.2)), 0.1, 4.0),
        "eig_y": jnp.clip(jnp.exp(math.log(4.0) - 3.6888794 * jax.random.uniform(arg_keys[4], (NY,), jnp.float32) ** levels(arg_keys[4], (NY,), ((0, 4),), -0.2, 0.2)), 0.1, 4.0),
        "eig_z": jnp.clip(jnp.exp(math.log(4.0) - 3.6888794 * jax.random.uniform(arg_keys[5], (KZ,), jnp.float32) ** levels(arg_keys[5], (KZ,), ((0, 2),), -0.2, 0.2)), 0.1, 4.0),
    }


def reference(rhs, basis_x, basis_y, eig_x, eig_y, eig_z):
    basis_xf = basis_x.astype(jnp.float32)
    basis_yf = basis_y.astype(jnp.float32)
    rhs_wide = rhs.astype(jnp.float32)
    section_g = jnp.einsum('xi,kxy->kiy', basis_xf, rhs_wide).astype(jnp.bfloat16)
    section_h = jnp.einsum('yj,kiy->kij', basis_yf, section_g.astype(jnp.float32))
    denominator = eig_z[:, None, None] + eig_x[None, :, None] + eig_y[None, None, :]
    scaled = (section_h / denominator).astype(jnp.bfloat16)
    section_v = jnp.einsum('yj,kij->kiy', basis_yf, scaled.astype(jnp.float32)).astype(jnp.bfloat16)
    section_s = jnp.einsum('xi,kiy->kxy', basis_xf, section_v.astype(jnp.float32))
    return section_s.astype(jnp.bfloat16), jnp.sum(rhs_wide * section_s)
```

```python
import jax
import jax.numpy as jnp
from jax import lax
from jax.sharding import PartitionSpec as P

F32, BF16 = jnp.float32, jnp.bfloat16
CHUNKS = 4


def distances(n):
    return [1 << b for b in range(n.bit_length() - 1)]


def swap(value, axis, n, d):
    return lax.ppermute(value, axis, [(s, s ^ d) for s in range(n)])


def with_swapped(value, axis, n, d, at):
    return jnp.stack([value, swap(value, axis, n, d)], axis=at)


def halves(value):
    cut = value.shape[0] // 2
    return value[:cut], value[cut:]


def dot(a, b, ca, cb):
    return lax.dot_general(a, b, (((ca,), (cb,)), ((), ())), preferred_element_type=F32)


def make(nx, ny, nz):
    near_x, near_y, near_z = distances(nx), distances(ny), distances(nz)
    far = ny // 2

    def shards(rhs, basis_x, basis_y, eig_x, eig_y, eig_z):
        p, z, k = (lax.axis_index(a) for a in ("gx", "gy", "gz"))
        field = rhs[0]
        lx, ly = basis_x.shape[1], basis_y.shape[1]
        own = lx // CHUNKS // nx

        def spread(order):
            places = [0]
            for d in reversed(order):
                places = places + [v + d for v in places]
            return places

        rows_x = basis_x.T
        orders, panels = [], []
        for m in range(CHUNKS):
            order = near_x if m % 2 == 0 else near_x[::-1]
            part = jnp.stack(
                [
                    lax.dynamic_slice_in_dim(rows_x, (m * nx + (p ^ d)) * own, own)
                    for d in spread(order)
                ]
            )
            at = 1
            for d in near_y[::-1]:
                part = with_swapped(part, "gy", ny, d, at)
                at += 1
            for d in near_z[::-1]:
                part = with_swapped(part, "gz", nz, d, at)
                at += 1
            orders.append(order)
            panels.append(part.reshape(-1, part.shape[-1]))

        def gathered(rows):
            for d in near_x:
                rows = jnp.concatenate([rows, swap(rows, "gx", nx, d)])
            for d in near_z:
                rows = jnp.concatenate([rows, swap(rows, "gz", nz, d)])
            return rows

        rows_y = basis_y.T
        here = gathered(rows_y)
        there = gathered(swap(rows_y, "gy", ny, far))

        all_x, all_y = eig_x, eig_y
        for d in near_x:
            all_x = jnp.concatenate([all_x, swap(all_x, "gx", nx, d)])
        for d in near_y:
            all_y = jnp.concatenate([all_y, swap(all_y, "gy", ny, d)])

        def piece(blocks, held, index, start, size):
            place = (index ^ (start // held)) * held + start % held
            return lax.dynamic_slice_in_dim(blocks, place, size)

        held_y = eig_y.shape[0]
        run_y = min(ly, held_y)
        values_y = jnp.concatenate(
            [
                piece(all_y, held_y, z, ((p ^ d) * nz + (k ^ e)) * ly + r, run_y)
                for e in range(nz)
                for d in range(nx)
                for r in range(0, ly, run_y)
            ]
        )
        values_y = values_y + eig_z[0]

        total = None
        energy = jnp.zeros((), F32)
        for m in range(CHUNKS):
            order, panel = orders[m], panels[m]
            keep, give = halves(panel)
            sent = swap(dot(give, field, 1, 0).astype(BF16), "gx", nx, order[0])
            g = dot(keep, field, 1, 0) + sent.astype(F32)
            for d in order[1:]:
                g, give = halves(g)
                g = g + swap(give.astype(BF16), "gx", nx, d).astype(F32)
            g = g.astype(BF16)

            g, give = halves(g)
            far_g = swap(give, "gy", ny, far)
            h = dot(g, here, 1, 1) + dot(far_g, there, 1, 1)
            for d in near_y[-2::-1]:
                h, give = halves(h)
                h = h + swap(give.astype(BF16), "gy", ny, d).astype(F32)
            values_x = jnp.concatenate(
                [
                    piece(
                        all_x,
                        eig_x.shape[0],
                        p,
                        (z * nz + (k ^ e)) * lx + (m * nx + p) * own,
                        own,
                    )
                    for e in range(nz)
                ]
            )
            w = (h / (values_x[:, None] + values_y[None, :])).astype(BF16)
            energy = energy + jnp.sum(h * w.astype(F32))

            for d in near_y[:-1]:
                w = jnp.concatenate([w, swap(w, "gy", ny, d)])
            far_v = swap(dot(w, there, 1, 0).astype(BF16), "gy", ny, far)
            v = jnp.concatenate([dot(w, here, 1, 0).astype(BF16), far_v])

            for d in order[:0:-1]:
                v = jnp.concatenate([v, swap(v, "gx", nx, d)])
            other = swap(v, "gx", nx, order[0])
            low, high = halves(panel)
            s = dot(low, v, 0, 0)
            total = s if total is None else total + s
            total = total + dot(high, other, 0, 0)
        for axis, n, near in (("gz", nz, near_z), ("gx", nx, near_x), ("gy", ny, near_y)):
            for d in near:
                energy = energy + swap(energy, axis, n, d)
        return total.astype(BF16)[None], energy

    return shards


def solution(mesh):
    nx, ny, nz = (mesh.shape[a] for a in ("gx", "gy", "gz"))
    return jax.shard_map(
        make(nx, ny, nz),
        mesh=mesh,
        in_specs=(
            P("gz", "gx", "gy"),
            P("gx", ("gy", "gz")),
            P("gy", ("gx", "gz")),
            P("gx"),
            P("gy"),
            P("gz"),
        ),
        out_specs=(P("gz", "gx", "gy"), P()),
        check_vma=False,
    )
```
